32 devices in a mesh: row: 8 (over z, x), col: 4 (over y, core).
Axes of the slice: x: 2, y: 2, z: 4, core: 2. Of those that a mesh axis runs over, the one named last changes fastest.
Arguments:
- coeffs: bfloat16 [1024, 128, 128], P(('row', 'col')), as said below
- tiles: int32 [1024, 1], replicated, may hold values from 0 to 7; in each aligned block of 32 rows (0 to 31, 32 to 63, ...) at most 5 rows name the same one
- primal: bfloat16 [1024, 1024], replicated, as said below
- dual_inverse: bfloat16 [1024, 1024], replicated, as said below
Outputs:
- schur: float32 [1024, 1024], P('row', 'col')
The draws below stay inside these ranges and needn't reach their ends.
Inputs may be any that keep to these rules, and one draw needn't show every extreme that they name: `tiles`: within each aligned block of 32 constraints (the constraints of one device) no tile is named more than 5 times, a bound that some block reaches. Each coeffs[i] is symmetric. `primal`: Symmetric. `dual_inverse`: Symmetric.
All inputs are finite; a program needn't handle non-finite values.
Results may differ from the reference program's by a relative error of at most 0.0022.
Values may be sent and summed in bfloat16 or wider, within the bound.
A program may use at most 128 MiB of HBM per device.

```python
import math
import jax
import jax.numpy as jnp
import numpy as np
from jax import lax

N = 1024
K = 128
CDEV = 32
NT = 8
MOST = 5
M = 1024


def symmetric_block(key, salt):
    value_key = jax.random.fold_in(key, salt)
    diagonal_key = jax.random.fold_in(key, salt + 1)
    raw_values = jnp.clip(jax.random.normal(value_key, (N, N), jnp.float32), -6.0, 6.0)
    matrix = (raw_values + raw_values.T) * 0.5 ** 0.5 / K ** 0.5
    matrix = matrix + jnp.diag(jax.random.uniform(diagonal_key, (N,), jnp.float32, 0.5, 1.5))
    return matrix.astype(jnp.bfloat16)


def draw_primal(key, part):
    return symmetric_block(key, 101)


def draw_dual_inverse(key, part):
    return symmetric_block(key, 211)


def draw_coeffs(key, part):
    value_key = jax.random.fold_in(key, 307)
    raw_values = jnp.clip(jax.random.normal(value_key, (M, K, K), jnp.float32), -6.0, 6.0)
    symmetric = (raw_values + jnp.swapaxes(raw_values, 1, 2)) * 0.5 ** 0.5 / K ** 0.5
    return symmetric.astype(jnp.bfloat16)


def shared_out(own_key, own, number, rows, count, top, bound, skew):
    ranking = jax.random.permutation(own_key, count)
    heavy_load, ordinary = shares(count, rows * top, bound, skew, True), shares(count, rows * top, bound, skew, False)
    places = jnp.arange(count)

    def named(tallies, offset_by):
        used = int((tallies > 0).sum())
        fixed = max(1, used // 4)
        passed = fixed + (places - fixed + offset_by * (used - fixed)) % max(1, count - fixed)
        return jnp.zeros((count,), jnp.int32).at[ranking[jnp.where(places < fixed, places, passed)]].set(jnp.asarray(tallies, jnp.int32))

    tallies = jnp.where(number % 4 == 0, named(heavy_load, number // 4), named(ordinary, number - number // 4 - 1))
    mixed = jax.random.permutation(jax.random.fold_in(own, 3), count)
    giver, receiver = mixed[0:count // 2 * 2:2], mixed[1:count // 2 * 2:2]
    slack = jnp.minimum(tallies[giver] - 1, bound - tallies[receiver]) // 2
    slack = jnp.where((giver == ranking[0]) | (receiver == ranking[0]) | (tallies[receiver] == 0), 0, jnp.maximum(slack, 0))
    passed = jax.random.randint(jax.random.fold_in(own, 4), (count // 2,), 0, 1 << 20) % (slack + 1)
    tallies = tallies.at[giver].add(-passed).at[receiver].add(passed)
    members = jnp.searchsorted(jnp.cumsum(tallies), jnp.arange(rows * top), side="right").astype(jnp.int32)
    table = members.reshape(top, rows).T
    table = table[jax.random.permutation(jax.random.fold_in(own, 1), rows)]
    offset_by = jax.random.randint(jax.random.fold_in(own, 2), (rows, 1), 0, top)
    return jnp.take_along_axis(table, (jnp.arange(top)[None, :] + offset_by) % top, axis=1)


def shares(amount, total, limit, skew, full):
    loads = [(1 << 20) // math.isqrt(grade ** skew) + 1 for grade in range(1, amount + 1)]
    largest = limit if full else min(limit, max(-(-total // amount), total * loads[0] // sum(loads)))
    least = 1 if total - largest >= amount - 1 else 0
    given, spare = [largest] + [least] * (amount - 1), total - largest - least * (amount - 1)
    while spare > 0:
        free = [i for i in range(1, amount) if given[i] < largest] or [i for i in range(1, amount) if given[i] < limit]
        mass, remaining = sum([loads[i] for i in free]), spare
        for i in free:
            more = min(limit - given[i], max(1, remaining * loads[i] // mass), spare)
            given[i] = given[i] + more
            spare = spare - more
    return np.array(given)


def setup_inputs(seed: int = 0) -> dict:
    splits = jax.random.split(jax.random.key(seed), 5)
    coeffs = draw_coeffs(jax.random.fold_in(splits[4], 71), 0)
    tiles_keys = jax.random.split(jax.random.fold_in(splits[1], 1), M // CDEV)
    tiles_turns = jax.random.permutation(jax.random.fold_in(splits[1], 3), M // CDEV)
    tiles = jax.vmap(lambda own, number: shared_out(jax.random.fold_in(splits[1], 2), own, number, CDEV, NT, 1, MOST, 2))(tiles_keys, tiles_turns).reshape((M, 1))
    primal = draw_primal(jax.random.fold_in(splits[4], 71), 0)
    dual_inverse = draw_dual_inverse(jax.random.fold_in(splits[4], 71), 0)
    return dict(coeffs=coeffs, tiles=tiles, primal=primal, dual_inverse=dual_inverse)


def slot_ranks(tile_group, first_tile, tile_width):
    labels = first_tile + jnp.arange(tile_width, dtype=jnp.int32)
    member = (tile_group[:, :, None] == labels[None, None, :]).astype(jnp.int32)
    before = jnp.cumsum(member, axis=1) - member
    return member, jnp.sum(before * member, axis=2)


def reference(coeffs, tiles, primal, dual_inverse):
    tile_count = N // K
    total = coeffs.shape[0]
    blocks = total // CDEV
    tile_area = K * K
    tile_ids = tiles[:, 0].astype(jnp.int32)
    member, ordinal = slot_ranks(tile_ids.reshape(blocks, CDEV), 0, tile_count)
    levels = jnp.arange(MOST, dtype=jnp.int32)
    chosen = member[:, :, :, None] * (ordinal[:, :, None, None] == levels[None, None, None, :]).astype(jnp.int32)
    offsets = jnp.arange(CDEV, dtype=jnp.int32)
    source = jnp.sum(chosen * offsets[None, :, None, None], axis=1)
    filled = jnp.sum(chosen, axis=1)
    anchor = (jnp.arange(blocks, dtype=jnp.int32)[:, None, None] * CDEV + source).reshape(-1).astype(jnp.int32)
    flat_coeffs = coeffs.reshape(total, tile_area).astype(jnp.float32)
    slot_rows = jnp.take(flat_coeffs, anchor, axis=0) * filled.reshape(-1, 1).astype(jnp.float32)
    slot_rows = slot_rows.reshape(blocks, tile_count, MOST, tile_area)
    position = (jnp.arange(blocks, dtype=jnp.int32)[:, None] * (tile_count * MOST)
                + tile_ids.reshape(blocks, CDEV) * MOST + ordinal).reshape(-1).astype(jnp.int32)
    primal_tiles = primal.reshape(tile_count, K, tile_count, K).astype(jnp.float32)
    dual_tiles = dual_inverse.reshape(tile_count, K, tile_count, K).astype(jnp.float32)
    block_rows = math.gcd(total, 64)

    def one_block(first_row):
        row_coeffs = lax.dynamic_slice_in_dim(coeffs, first_row, block_rows, 0).astype(jnp.float32)
        row_tiles = lax.dynamic_slice_in_dim(tile_ids, first_row, block_rows, 0)
        primal_pick = jnp.take(primal_tiles, row_tiles, axis=0)
        product_tile = jnp.einsum("iab,ibuc->iuac", row_coeffs, primal_pick).astype(jnp.bfloat16)
        dual_pick = jnp.take(dual_tiles, row_tiles, axis=2)
        reduced = jnp.einsum("iuba,ucib->iuac", product_tile.astype(jnp.float32), dual_pick).astype(jnp.bfloat16)
        reduced = reduced.reshape(block_rows, tile_count, tile_area).astype(jnp.float32)
        values = jnp.einsum("iux,suqx->isuq", reduced, slot_rows).reshape(block_rows, -1)
        return jnp.take(values, position, axis=1)

    starts = jnp.arange(0, total, block_rows, dtype=jnp.int32)
    return lax.map(one_block, starts).reshape(total, total)
```

```python
import functools

import jax
import jax.numpy as jnp
from jax import lax
from jax.experimental import pallas as pl
from jax.experimental.pallas import tpu as pltpu
from jax.sharding import PartitionSpec as P

MOST = 5
CORES = 2
STEP = 4
GROUP = 16
MESH = pl.DeviceIdType.MESH


def slot_ranks(tile_group, first_tile, tile_width):
    labels = first_tile + jnp.arange(tile_width, dtype=jnp.int32)
    member = (tile_group[:, :, None] == labels[None, None, :]).astype(jnp.int32)
    before = jnp.cumsum(member, axis=1) - member
    return (member, jnp.sum(before * member, axis=2))


def fast_size(row_size):
    fast = 1
    while (2 * fast) * (2 * fast) <= row_size:
        fast *= 2
    return fast


def kernel(
    fast, tiles_ref, coeffs_ref, routed_ref, right_ref, left_ref,
    cols_ref, rows_ref, packed_ref,
    stage, col_recv, row_recv, local_sem, route_send, row_send, pass_send,
    up_send, down_send, plus_send, minus_send,
):
    row_size = lax.axis_size("row")
    col_size = lax.axis_size("col")
    slow = row_size // fast
    r = lax.axis_index("row")
    c = lax.axis_index("col")
    a = r // fast
    b = r % fast
    own = coeffs_ref.shape[0]
    size = coeffs_ref.shape[1]
    half = size // 2
    width = right_ref.shape[1]
    y_size = col_size // CORES
    y = c // CORES
    core = c % CORES

    def source(j):
        return ((y + j // CORES) % y_size) * CORES + (core + j % CORES) % CORES

    partner = y * CORES + (core + 1) % CORES

    barrier = pltpu.get_barrier_semaphore()
    for j in range(1, col_size):
        pl.semaphore_signal(barrier, inc=1, device_id=(r, source(j)), device_id_type=MESH)
    has_up, has_down = a < slow - 1, a > 0
    has_plus, has_minus = b < fast - 1, b > 0
    moves = [(has_up, r + fast), (has_down, r - fast), (has_plus, r + 1), (has_minus, r - 1)]
    for exists, there in moves:
        @pl.when(exists)
        def _():
            pl.semaphore_signal(barrier, inc=1, device_id=(there, c), device_id_type=MESH)
    near = sum(exists.astype(jnp.int32) for exists, _ in moves)
    pl.semaphore_wait(barrier, near + (col_size - 1))

    def remote(src, dst, send, recv, there):
        return pltpu.make_async_remote_copy(
            src_ref=src, dst_ref=dst, send_sem=send, recv_sem=recv,
            device_id=there, device_id_type=MESH,
        )

    finish = []

    routes = []
    for j in range(1, col_size):
        target = source(j)
        copy = remote(
            routed_ref.at[target], cols_ref.at[r, c], route_send.at[j],
            col_recv.at[r, c], (r, target),
        )
        copy.start()
        finish.append((None, copy))
    keep_cols = pltpu.make_async_copy(routed_ref.at[c], cols_ref.at[r, c], local_sem.at[0])
    keep_cols.start()
    keep_rows = pltpu.make_async_copy(coeffs_ref, rows_ref.at[c], local_sem.at[1])
    keep_rows.start()
    for j in range(1, col_size):
        if j == 1 or j % CORES == 0:
            copy = remote(
                coeffs_ref, rows_ref.at[c], row_send.at[j], row_recv.at[c], (r, source(j))
            )
            copy.start()
            finish.append((None, copy))

    def piece_wait(there_r, there_c):
        remote(
            cols_ref.at[there_r, there_c], cols_ref.at[there_r, there_c],
            local_sem.at[2], col_recv.at[there_r, there_c], (r, partner),
        ).wait_recv()

    def piece_send(valid, exists, there, pr, pc, send):
        copy = remote(
            cols_ref.at[pr, pc], cols_ref.at[pr, pc], send, col_recv.at[pr, pc], (there, c)
        )
        cond = exists if valid is None else jnp.logical_and(valid, exists)

        @pl.when(cond)
        def _():
            copy.start()

        finish.append((cond, copy))

    def handle(d, sign, j):
        pr = r - sign * d * fast
        pc = source(j)
        if d == 0:
            valid = None
            if j == 0:
                keep_cols.wait()
            else:
                piece_wait(pr, pc)
        else:
            valid = (a - d >= 0) if sign > 0 else (a + d < slow)

            @pl.when(valid)
            def _():
                piece_wait(pr, pc)
        k = (d if sign > 0 else d + slow - 1) * col_size + j
        if d == 0 or sign > 0:
            if d < slow - 1:
                piece_send(valid, has_up, r + fast, pr, pc, up_send.at[d * col_size + j])
        if d == 0 or sign < 0:
            if d < slow - 1:
                piece_send(valid, has_down, r - fast, pr, pc, down_send.at[d * col_size + j])
        piece_send(valid, has_plus, r + 1, pr, pc, plus_send.at[k])
        piece_send(valid, has_minus, r - 1, pr, pc, minus_send.at[k])

    events = [functools.partial(handle, 0, 1, j) for j in range(col_size)]
    for d in range(1, slow):
        for j in range(col_size):
            events.append(functools.partial(handle, d, 1, j))
            events.append(functools.partial(handle, d, -1, j))

    def cross(e, sign, ap, j):
        pr = ap * fast + b - sign * e
        pc = source(j)
        valid = (b - e >= 0) if sign > 0 else (b + e < fast)

        @pl.when(valid)
        def _():
            piece_wait(pr, pc)
        k = (2 * slow - 1) * col_size + ((e - 1) * slow + ap) * col_size + j
        if e < fast - 1:
            if sign > 0:
                piece_send(valid, has_plus, r + 1, pr, pc, plus_send.at[k])
            else:
                piece_send(valid, has_minus, r - 1, pr, pc, minus_send.at[k])

    crossings = []
    for e in range(1, fast):
        for ap in range(slow):
            for j in range(col_size):
                crossings.append(functools.partial(cross, e, 1, ap, j))
                crossings.append(functools.partial(cross, e, -1, ap, j))

    line = lax.broadcasted_iota(jnp.int32, (half, size), 0)
    lane = lax.broadcasted_iota(jnp.int32, (half, size), 1)
    left = lane < half
    below = jnp.logical_or(left, lane - half <= line)
    scale = jnp.where(lane - half == line, 0.5, 1.0).astype(jnp.float32)
    corner = jnp.where(lane == line, 0.5, 0.0).astype(jnp.float32)
    pitch = half + 8

    def row_step(pc, first):
        def body(n, carry):
            i = first + n
            t = tiles_ref[(r * col_size + pc) * own + i]
            block = rows_ref[pc, i]
            slot = lax.rem(i, GROUP)
            for u in range(width):
                w = jnp.dot(block, right_ref[t, u], preferred_element_type=jnp.float32)
                w = w.astype(jnp.bfloat16)
                w = jnp.concatenate([w[:, size:], w[:, :size]], axis=0)
                total = jnp.dot(left_ref[t, u], w, preferred_element_type=jnp.float32)
                top, bottom = total[:half], total[half:]
                main = jnp.where(below, bottom, pltpu.roll(top, half, 1)) * scale
                base = pl.multiple_of(slot * pitch, 8)
                stage[u, pl.ds(base, half), :] = main
                diag = jnp.sum(top * corner, axis=0, keepdims=True)
                stage[u, pl.ds(base + half, 8), :] = jnp.broadcast_to(diag, (8, size))
            return carry

        lax.fori_loop(0, STEP, body, 0)

    def row_flush(pc, first):
        start = pl.multiple_of(pc * own + first, GROUP)
        for u in range(width):
            for k in range(half + 1):
                part = stage[u, pl.ds(k, GROUP, stride=pitch), :]
                packed_ref[u, k, pl.ds(start, GROUP), :] = part.astype(jnp.bfloat16)

    def rows_ready(j):
        pc = source(j)
        if j == 0:
            keep_rows.wait()
            return
        copy = remote(
            rows_ref.at[pc], rows_ref.at[pc], pass_send.at[j], row_recv.at[pc], (r, partner)
        )
        copy.wait_recv()
        if j % CORES == 0:
            copy.start()
            finish.append((None, copy))

    work = []
    for j in range(col_size):
        work.append(functools.partial(rows_ready, j))

        def group(n, j=j):
            first = n * GROUP
            for s in range(0, GROUP, STEP):
                row_step(source(j), first + s)
            row_flush(source(j), first)

        for n in range(own // GROUP):
            first = n * GROUP
            for s in range(0, GROUP, STEP):
                work.append(functools.partial(row_step, source(j), first + s))
            work.append(functools.partial(row_flush, source(j), first))

    done = 0
    for k, event in enumerate(events):
        event()
        upto = len(work) * max(0, k + 1 - col_size // 2) // (len(events) - col_size // 2)
        while done < upto:
            work[done]()
            done += 1
    for event in crossings:
        event()
    for cond, copy in finish:
        if cond is None:
            copy.wait_send()
        else:
            pl.when(cond)(copy.wait_send)


def gather_and_reduce(fast, tile_ids, coeffs, routed, right, left):
    row_size = lax.axis_size("row")
    col_size = lax.axis_size("col")
    own, size, _ = coeffs.shape
    width = right.shape[1]
    slow = row_size // fast
    crossed = ((2 * slow - 1) + (fast - 1) * slow) * col_size
    vmem = pl.BlockSpec(memory_space=pltpu.VMEM)
    dma = pltpu.SemaphoreType.DMA
    return pl.pallas_call(
        functools.partial(kernel, fast),
        out_shape=(
            jax.ShapeDtypeStruct((row_size, col_size) + routed.shape[1:], jnp.bfloat16),
            jax.ShapeDtypeStruct((col_size,) + coeffs.shape, jnp.bfloat16),
            jax.ShapeDtypeStruct((width, size // 2 + 1, col_size * own, size), jnp.bfloat16),
        ),
        in_specs=[pl.BlockSpec(memory_space=pltpu.SMEM)] + [vmem] * 4,
        out_specs=(vmem, vmem, vmem),
        scratch_shapes=[
            pltpu.VMEM((width, GROUP * (size // 2 + 8), size), jnp.float32),
            dma((row_size, col_size)),
            dma((col_size,)),
            dma((3,)),
            dma((col_size,)),
            dma((col_size,)),
            dma((col_size,)),
            dma((slow * col_size,)),
            dma((slow * col_size,)),
            dma((crossed,)),
            dma((crossed,)),
        ],
        compiler_params=pltpu.CompilerParams(
            collective_id=0, has_side_effects=True, vmem_limit_bytes=60 * 1024 * 1024
        ),
    )(tile_ids, coeffs, routed, right, left)


def shards(coeffs, tiles, primal, dual_inverse):
    col_size = lax.axis_size("col")
    row_size = lax.axis_size("row")
    col_index = lax.axis_index("col")
    row_index = lax.axis_index("row")
    own, size, _ = coeffs.shape
    half = size // 2
    tile_count = primal.shape[0] // size
    per_col = tile_count // col_size
    slots = per_col * MOST
    tile_ids = tiles[:, 0]
    row_count = col_size * own
    first_tile = col_index * per_col

    line = lax.broadcasted_iota(jnp.int32, (half, size), 0)
    lane = lax.broadcasted_iota(jnp.int32, (half, size), 1)
    below = jnp.logical_or(lane < half, lane - half <= line)
    shifted = jnp.concatenate([coeffs[:, :half, half:], coeffs[:, :half, :half]], axis=2)
    main = jnp.where(below, coeffs[:, half:, :], shifted)
    corner = (lane == line).astype(coeffs.dtype)
    diag = jnp.sum(coeffs[:, :half, :] * corner, axis=1)
    own_tiles = lax.dynamic_slice_in_dim(tile_ids, (row_index * col_size + col_index) * own, own)
    member, ordinal = slot_ranks(own_tiles[None], 0, tile_count)
    levels = jnp.arange(MOST, dtype=jnp.int32)
    chosen = member[0][:, :, None] * (ordinal[0][:, None, None] == levels).astype(jnp.int32)
    offsets = jnp.arange(own, dtype=jnp.int32)
    origin = jnp.sum(chosen * offsets[:, None, None], axis=0).reshape(-1)
    main = jnp.take(main, origin, axis=0).reshape(col_size, slots * half, size)
    diag = jnp.take(diag, origin, axis=0).reshape(col_size, slots, size)
    extra = -(-slots // 16) * 16
    diag = jnp.pad(diag, ((0, 0), (0, extra - slots), (0, 0)))
    fill = -(slots * half) % 16
    routed = jnp.concatenate([main, diag], axis=1)
    routed = jnp.pad(routed, ((0, 0), (0, fill), (0, 0)))

    def strip(matrix):
        part = lax.dynamic_slice_in_dim(matrix, first_tile * size, per_col * size, 0)
        part = part.reshape(per_col, size, tile_count, size)
        return jnp.transpose(part, (2, 0, 1, 3))

    def stripe(matrix):
        part = lax.dynamic_slice_in_dim(matrix, first_tile * size, per_col * size, 1)
        part = part.reshape(tile_count, size, per_col, size)
        return jnp.transpose(part, (0, 2, 1, 3))

    left = jnp.concatenate([strip(primal), strip(dual_inverse)], axis=3)
    right = jnp.concatenate([stripe(primal), stripe(dual_inverse)], axis=3)
    cols, _, packed = gather_and_reduce(
        fast_size(row_size), tile_ids, coeffs, routed, right, left
    )
    main = cols[:, :, : slots * half].reshape(
        row_size * col_size, per_col, MOST, half, size
    )
    diag = cols[:, :, slots * half : slots * (half + 1)].reshape(
        row_size * col_size, per_col, MOST, size
    )
    values = jnp.einsum(
        "vaib,gvqab->igvq", packed[:, :half], main, preferred_element_type=jnp.float32
    ) + jnp.einsum("vib,gvqb->igvq", packed[:, half], diag, preferred_element_type=jnp.float32)
    home_span = row_size * slots
    values = values.reshape(row_count, col_size, home_span)
    landed = lax.all_to_all(values, "col", split_axis=1, concat_axis=1, tiled=True)
    landed = landed.reshape(row_count, col_size * home_span)
    home_tiles = lax.dynamic_slice_in_dim(
        tile_ids, col_index * row_size * own, row_size * own
    )
    home_tiles = home_tiles.reshape(row_size, own)
    _, ordinal = slot_ranks(home_tiles, 0, tile_count)
    owner_col = home_tiles // per_col
    within = home_tiles - owner_col * per_col
    sender = jnp.arange(row_size, dtype=jnp.int32)[:, None]
    column_pick = owner_col * home_span + sender * slots + within * MOST + ordinal
    pick = column_pick.reshape(1, -1) == jnp.arange(col_size * home_span, dtype=jnp.int32)[:, None]
    return jnp.dot(landed, pick.astype(jnp.float32), precision=lax.Precision.HIGHEST)


def solution(mesh):
    return jax.shard_map(
        shards,
        mesh=mesh,
        in_specs=(P(("row", "col"), None, None), P(), P(), P()),
        out_specs=P("row", "col"),
        check_vma=False,
    )
```
